1024 devices in a mesh: ctx: 32 (over z), ep: 32 (over x, y, core).
Axes of the slice: x: 4, y: 4, z: 32, core: 2. Of those that a mesh axis runs over, the one named last changes fastest.
Arguments:
- out_grad: bfloat16 [2048, 3584], P(('ctx', 'ep')), may hold values from -6 to 6
- expert_ids: int32 [2048, 8], P(('ctx', 'ep')), may hold values from 0 to 127, all different within a row; in each aligned block of 64 rows (0 to 63, 64 to 127, ...) at most 7 rows name the same one
- gate_values: float32 [2048, 8], P(('ctx', 'ep')), may hold values from 0.1 to 2.5
- hidden: bfloat16 [32, 128, 7, 1536], P(None, 'ep', None, 'ctx'), may hold values from -0.29882812 to 0.29882812
- w_down: bfloat16 [128, 1536, 3584], P('ep', 'ctx'), may hold values from -0.15625 to 0.15625
Outputs:
- hidden_grad: bfloat16 [32, 128, 7, 1536], P(None, 'ep', None, 'ctx')
- weight_grad: bfloat16 [128, 1536, 3584], P('ep', 'ctx')
- gate_grad: float32 [2048, 8], P(('ctx', 'ep'))
The draws below stay inside these ranges and needn't reach their ends.
Inputs may be any that keep to these rules, and one draw needn't show every extreme that they name: `expert_ids`: each token names 8 different experts. In each aligned block of 64 tokens no expert is named by more than 7 tokens.
All inputs are finite; a program needn't handle non-finite values.
Results may differ from the reference program's by a relative error of at most 0.012.
Values may be sent and summed in bfloat16 or wider, within the bound.
A program may use at most 64 MiB of HBM per device.

```python
import math
import jax
import jax.numpy as jnp
import numpy as np
from jax import lax

D = 3584
F = 1536
TOPK = 8
EXPERTS = 128
CAPACITY = 7
GROUPS = 32
GROUP_TOK = 64
TOKENS = 2048


def level_of(stream_key, extent, pieces, low, high):
    factor_of, own = 1.0, jax.random.fold_in(stream_key, 6)
    for axis_at, parts in pieces:
        heights = jnp.exp(jax.random.uniform(jax.random.fold_in(own, axis_at), (parts,), jnp.float32, low / len(pieces), high / len(pieces)))
        factor_of = factor_of * jnp.repeat(heights, extent[axis_at] // parts).reshape([-1 if axis == axis_at else 1 for axis in range(len(extent))])
    return factor_of


def routed_block(key, own, number, rows, amount, top, most, lean):
    order = jax.random.permutation(key, amount)
    heavy_load, common = portions_of(amount, rows * top, most, lean, True), portions_of(amount, rows * top, most, lean, False)
    places = jnp.arange(amount)

    def named(tallies, offset_by):
        used = int((tallies > 0).sum())
        fixed = max(1, used // 4)
        moved = fixed + (places - fixed + offset_by * (used - fixed)) % max(1, amount - fixed)
        return jnp.zeros((amount,), jnp.int32).at[order[jnp.where(places < fixed, places, moved)]].set(jnp.asarray(tallies, jnp.int32))

    tallies = jnp.where(number % 4 == 0, named(heavy_load, number // 4), named(common, number - number // 4 - 1))
    mixed = jax.random.permutation(jax.random.fold_in(own, 3), amount)
    donor, sink = mixed[0:amount // 2 * 2:2], mixed[1:amount // 2 * 2:2]
    room = jnp.minimum(tallies[donor] - 1, most - tallies[sink]) // 2
    room = jnp.where((donor == order[0]) | (sink == order[0]) | (tallies[sink] == 0), 0, jnp.maximum(room, 0))
    moved = jax.random.randint(jax.random.fold_in(own, 4), (amount // 2,), 0, 1 << 20) % (room + 1)
    tallies = tallies.at[donor].add(-moved).at[sink].add(moved)
    labels = jnp.searchsorted(jnp.cumsum(tallies), jnp.arange(rows * top), side="right").astype(jnp.int32)
    table = labels.reshape(top, rows).T
    table = table[jax.random.permutation(jax.random.fold_in(own, 1), rows)]
    offset_by = jax.random.randint(jax.random.fold_in(own, 2), (rows, 1), 0, top)
    return jnp.take_along_axis(table, (jnp.arange(top)[None, :] + offset_by) % top, axis=1)


def portions_of(number_of, total, most, slope, full):
    portions = [(1 << 20) // math.isqrt(standing ** slope) + 1 for standing in range(1, number_of + 1)]
    largest = most if full else min(most, max(-(-total // number_of), total * portions[0] // sum(portions)))
    least = 1 if total - largest >= number_of - 1 else 0
    counts, surplus = [largest] + [least] * (number_of - 1), total - largest - least * (number_of - 1)
    while surplus > 0:
        movable = [i for i in range(1, number_of) if counts[i] < largest] or [i for i in range(1, number_of) if counts[i] < most]
        mass, remaining = sum([portions[i] for i in movable]), surplus
        for i in movable:
            extra = min(most - counts[i], max(1, remaining * portions[i] // mass), surplus)
            counts[i] = counts[i] + extra
            surplus = surplus - extra
    return np.array(counts)


def scatter_about(stream_key, dims, spread, bound, shards=(), kind=jnp.bfloat16):
    values = spread * jax.random.normal(stream_key, dims, jnp.float32)
    if shards:
        values = values * level_of(stream_key, dims, shards, -0.22, 0.18)
    return jnp.clip(values, -bound, bound).astype(kind)


def setup_inputs(seed: int = 0) -> dict:
    splits = jax.random.split(jax.random.key(seed), 6)
    out_grad = scatter_about(splits[0], (TOKENS, D), 1.0, 6.0, ((0, 1024),))
    expert_ids_keys = jax.random.split(jax.random.fold_in(splits[1], 1), TOKENS // GROUP_TOK)
    expert_ids_turns = jax.random.permutation(jax.random.fold_in(splits[1], 3), TOKENS // GROUP_TOK)
    expert_ids = jax.vmap(lambda own, number: routed_block(jax.random.fold_in(splits[1], 2), own, number, GROUP_TOK, EXPERTS, TOPK, CAPACITY, 2))(expert_ids_keys, expert_ids_turns).reshape((TOKENS, TOPK))
    gate_values = jnp.clip(jnp.exp(math.log(2.5) - 3.218876 * jax.random.uniform(splits[2], (TOKENS, TOPK), jnp.float32) ** level_of(splits[2], (TOKENS, TOPK), ((0, 1024),), -0.2, 0.2)), 0.1, 2.5)
    hidden = scatter_about(splits[3], (GROUPS, EXPERTS, CAPACITY, F), 0.05, 0.29882812, ((1, 32), (3, 32)))
    w_down = scatter_about(splits[4], (EXPERTS, F, D), F ** -0.5, 0.15625, ((0, 32), (1, 32)))
    return {"out_grad": out_grad, "expert_ids": expert_ids, "gate_values": gate_values, "hidden": hidden, "w_down": w_down}


def route_slots(expert_ids):
    group_routes = GROUP_TOK * TOPK
    group_ids = expert_ids.reshape(GROUPS, group_routes)
    onehot = (group_ids[:, :, None] == jnp.arange(EXPERTS, dtype=jnp.int32)[None, None, :]).astype(jnp.int32)
    before = jnp.cumsum(onehot, axis=1) - onehot
    slot_index = jnp.sum(before * onehot, axis=2).astype(jnp.int32)
    return group_ids, slot_index


def reference(out_grad, expert_ids, gate_values, hidden, w_down):
    group_routes = GROUP_TOK * TOPK
    group_ids, slot_index = route_slots(expert_ids)
    place = (group_ids * CAPACITY + slot_index).astype(jnp.int32)
    group_base = (jnp.arange(GROUPS, dtype=jnp.int32) * GROUP_TOK)[:, None]
    token_index = group_base + (jnp.arange(group_routes, dtype=jnp.int32) // TOPK)[None, :]
    group_index = jnp.broadcast_to(jnp.arange(GROUPS, dtype=jnp.int32)[:, None], place.shape)
    slot_token = jnp.zeros((GROUPS, EXPERTS * CAPACITY), jnp.int32).at[group_index, place].set(token_index + 1)
    slot_gate = jnp.zeros((GROUPS, EXPERTS * CAPACITY), jnp.float32).at[group_index, place].set(
        gate_values.reshape(GROUPS, group_routes))
    slot_token = slot_token.reshape(GROUPS, EXPERTS, CAPACITY)
    slot_gate = slot_gate.reshape(GROUPS, EXPERTS, CAPACITY)

    def one_expert(expert):
        token_pick = slot_token[:, expert, :].reshape(-1)
        gate_pick = slot_gate[:, expert, :].reshape(-1)
        live_mask = token_pick > 0
        safe_index = jnp.maximum(token_pick - 1, 0).astype(jnp.int32)
        slot_rows = jnp.where(live_mask[:, None], out_grad[safe_index], jnp.zeros((), out_grad.dtype))
        weight = w_down[expert]
        grad_in = jnp.dot(slot_rows, weight.T, preferred_element_type=jnp.float32)
        saved_hid = hidden[:, expert].reshape(GROUPS * CAPACITY, F)
        hid_grad = (gate_pick[:, None] * grad_in).astype(jnp.bfloat16)
        gate_slot = jnp.sum(saved_hid.astype(jnp.float32) * grad_in, axis=1)
        scaled = (gate_pick[:, None] * slot_rows.astype(jnp.float32)).astype(jnp.bfloat16)
        weight_sum = jnp.dot(saved_hid.T, scaled, preferred_element_type=jnp.float32)
        return hid_grad.reshape(GROUPS, CAPACITY, F), gate_slot.reshape(GROUPS, CAPACITY), weight_sum.astype(jnp.bfloat16)

    hid_all, gate_all, weight_grad = lax.map(one_expert, jnp.arange(EXPERTS, dtype=jnp.int32))
    hidden_grad = jnp.transpose(hid_all, (1, 0, 2, 3))
    gate_table = jnp.transpose(gate_all, (1, 0, 2)).reshape(GROUPS, EXPERTS * CAPACITY)
    gate_grad = jnp.take_along_axis(gate_table, place, axis=1).reshape(TOKENS, TOPK)
    return hidden_grad, weight_grad, gate_grad
```

```python
import functools

import jax
import jax.numpy as jnp
from jax import lax
from jax.experimental import pallas as pl
from jax.experimental.pallas import tpu as pltpu
from jax.sharding import PartitionSpec as P

MESH = pl.DeviceIdType.MESH
F32, BF16 = jnp.float32, jnp.bfloat16

NZ = 32
NE = 32
CHUNKS, PER = 8, 4
LANES = 3584 + 128
COLOURS = (
    ((0, 1920), (0, 1024), (1024, 896)),
    ((1920, 1792), (1920, 896), (2816, 896)),
)


def kernel(
    own_ref, hid_ref, w_ref,
    hg_ref, dw_ref, val_ref,
    zbuf, xall, dwacc, msg, rbuf, fbuf,
    zs_sem, zr_sem, s_sem, r_sem, d_sem, ms_sem, mr_sem, fs_sem, fr_sem,
):
    z, ep = lax.axis_index("ctx"), lax.axis_index("ep")
    core, px, py = ep % 2, ep // 8, (ep // 2) % 4
    experts, capacity = 4, hid_ref.shape[1]
    width = w_ref.shape[0]
    part = width // experts
    model = w_ref.shape[1]

    def along_z(d):
        return ((z + d + NZ) % NZ, ep)

    def chip(x, y):
        return ((x + 4) % 4 * 4 + (y + 4) % 4) * 2 + core

    def at(colour, dp, dq):
        return chip(px + dq, py + dp) if colour == 0 else chip(px + dp, py + dq)

    partner = (z, ep + 1 - 2 * core)

    barrier = pltpu.get_barrier_semaphore()
    near = [along_z(d) for d in (1, 2, 3, 4, -1, -2, -3, -4)]
    near += [(z, at(0, 1, 0)), (z, at(0, -1, 0)), (z, at(0, 0, 1)), (z, at(0, 0, -1)), partner]
    for peer in near:
        pl.semaphore_signal(barrier, inc=1, device_id=peer, device_id_type=MESH)
    pl.semaphore_wait(barrier, len(near))

    def z_send(src, slot, d):
        pltpu.make_async_remote_copy(
            src_ref=src, dst_ref=zbuf.at[slot], send_sem=zs_sem.at[0], recv_sem=zr_sem.at[slot],
            device_id=along_z(d), device_id_type=MESH,
        ).start()

    for j in (4, 3, 2, 1):
        z_send(own_ref, j - 1, j)
        z_send(own_ref, 16 + j, -j)
    zbuf[16] = own_ref[...]
    dwacc[...] = jnp.zeros_like(dwacc)

    def z_wait(slot):
        pltpu.make_async_copy(own_ref, zbuf.at[slot], zr_sem.at[slot]).wait()

    def chunk_of(n):
        up = 1 - n % 2
        return 4 * up + n // 2, up, n // 2

    def group_of(n, i):
        _, up, w = chunk_of(n)
        return (z + 2 * NZ + up * (4 * w + i) - (1 - up) * (4 * w + i + 1)) % NZ

    def fetch(n):
        c, up, w = chunk_of(n)

        @pl.when(up == 1)
        def _():
            @pl.when(w > 0)
            def _():
                z_wait(16 + 4 * w)
                for j in (4, 3, 2, 1):
                    if j < 4:
                        z_send(zbuf.at[16 + 4 * w], 16 + 4 * w + j, -j)
                    else:
                        @pl.when(w < 3)
                        def _():
                            z_send(zbuf.at[16 + 4 * w], 16 + 4 * w + 4, -4)
            for i in (1, 2, 3):
                z_wait(16 + 4 * w + i)

        @pl.when(up == 0)
        def _():
            z_wait(4 * w + 3)

            @pl.when(w < 3)
            def _():
                for j in (4, 3, 2, 1):
                    z_send(zbuf.at[4 * w + 3], 4 * w + 3 + j, j)
            for i in (0, 1, 2):
                z_wait(4 * w + i)

        rows = [zbuf[4 * c + i].astype(F32) for i in range(PER)]
        xall[c, ep] = jnp.concatenate(rows, axis=0).astype(BF16)

    def block(c, e, lanes):
        return xall.at[c, e, :, pl.ds(*lanes)]

    def send(c, e, lanes, to, sem):
        pltpu.make_async_remote_copy(
            src_ref=block(c, e, lanes), dst_ref=block(c, e, lanes), send_sem=s_sem.at[c], recv_sem=sem,
            device_id=to, device_id_type=MESH,
        ).start()

    def share(c, colour, dp, dq):
        send(c, at(colour, dp, dq), COLOURS[colour][0], partner, d_sem.at[c])

    def send_p(c, colour, dp, dq, step, piece):
        send(c, at(colour, dp, dq), COLOURS[colour][piece], (z, at(colour, step, 0)),
             r_sem.at[c, colour, (dp - step) % 4 * 4 + dq % 4])

    def send_q(c, colour, dp, dq, step, piece):
        send(c, at(colour, dp, dq), COLOURS[colour][piece], (z, at(colour, 0, step)),
             r_sem.at[c, colour, dp % 4 * 4 + (dq - step) % 4])

    def wait(c, colour, dp, dq):
        ref = block(c, at(colour, dp, dq), COLOURS[colour][0])
        pltpu.make_async_copy(ref, ref, r_sem.at[c, colour, dp % 4 * 4 + dq % 4]).wait()

    def stage1(c):
        for colour in (0, 1):
            send_p(c, colour, 0, 0, 1, 0)
            send_p(c, colour, 0, 0, -1, 0)
        for colour in (0, 1):
            share(c, colour, 0, 0)

    def stage2(c):
        for colour in (0, 1):
            for dp in (-1, 1):
                wait(c, colour, dp, 0)
                send_p(c, colour, dp, 0, -dp, 1 if dp < 0 else 2)
        for colour in (0, 1):
            for dp in (0, -1, 1):
                send_q(c, colour, dp, 0, 1, 0)
                send_q(c, colour, dp, 0, -1, 0)
        for colour in (0, 1):
            for dp in (-1, 1):
                share(c, colour, dp, 0)

    def stage3(c):
        for colour in (0, 1):
            wait(c, colour, 2, 0)
            send_q(c, colour, 2, 0, 1, 0)
            send_q(c, colour, 2, 0, -1, 0)
        for dp in (0, -1, 1):
            for colour in (0, 1):
                for dq in (-1, 1):
                    wait(c, colour, dp, dq)
                    send_q(c, colour, dp, dq, -dq, 1 if dq < 0 else 2)
        for colour in (0, 1):
            share(c, colour, 2, 0)
            for dp in (0, -1, 1):
                for dq in (-1, 1):
                    share(c, colour, dp, dq)

    def stage4(c):
        for colour in (0, 1):
            for dq in (-1, 1):
                wait(c, colour, 2, dq)
                send_q(c, colour, 2, dq, -dq, 1 if dq < 0 else 2)
        for colour in (0, 1):
            for dp in (0, -1, 1):
                wait(c, colour, dp, 2)
                share(c, colour, dp, 2)
            for dq in (-1, 1):
                share(c, colour, 2, dq)

    def stage5(c):
        for colour in (0, 1):
            wait(c, colour, 2, 2)
            share(c, colour, 2, 2)

    rows256 = NE * 2 * PER

    def compute(n):
        c, _, _ = chunk_of(n)
        half = xall.at[c, pl.ds(0, NE // 2)]
        pltpu.make_async_copy(half, half, d_sem.at[c]).wait()
        gates = xall[c, :, :, pl.ds(model, 128)].reshape(rows256, 128)
        e_at = lax.broadcasted_iota(jnp.int32, (128, width), 0)
        f_at = lax.broadcasted_iota(jnp.int32, (128, width), 1)
        pick = jnp.where(e_at == experts * ep + f_at // part, 1.0, 0.0).astype(BF16)
        gate = jnp.dot(gates, pick, preferred_element_type=F32)
        live = gate > 0
        r_at = lax.broadcasted_iota(jnp.int32, (rows256, rows256), 0)
        c_at = lax.broadcasted_iota(jnp.int32, (rows256, rows256), 1)
        earlier = ((r_at % 8) // 2 == (c_at % 8) // 2) & (c_at < r_at)
        slot = jnp.dot(
            jnp.where(earlier, 1.0, 0.0).astype(BF16), jnp.where(live, 1.0, 0.0).astype(BF16),
            preferred_element_type=F32,
        )
        slot = jnp.where(live, slot, -1.0).reshape(NE, 8, width)
        rows = xall[c, :, :, pl.ds(0, model)].reshape(rows256, model)
        grad_in = lax.dot_general(rows, w_ref[...], (((1,), (1,)), ((), ())), preferred_element_type=F32)
        own_group = [hid_ref[group_of(n, i)].astype(F32) for i in range(PER)]
        row8 = lax.broadcasted_iota(jnp.int32, (8, width), 0) // 2
        hid = jnp.zeros((NE, 8, width), F32)
        for s in range(capacity):
            wide = jnp.zeros((8, width), F32)
            for i in range(PER):
                wide = jnp.where(row8 == i, own_group[i][s : s + 1, :], wide)
            hid = jnp.where(slot == float(s), wide[None], hid)
        grad3 = grad_in.reshape(NE, 8, width)
        gate3 = gate.reshape(NE, 8, width)
        out = (gate3 * grad3).astype(BF16).astype(F32)
        term = hid * grad3
        terms = []
        outs = []
        for s in range(capacity):
            here = slot == float(s)
            o = jnp.sum(jnp.where(here, out, 0.0), axis=0)
            t = jnp.sum(jnp.where(here, term, 0.0), axis=0)
            outs.append(o + pltpu.roll(o, 7, 0))
            terms.append(t + pltpu.roll(t, 7, 0))
        for i in range(PER):
            hg_ref[group_of(n, i)] = jnp.concatenate([o[2 * i : 2 * i + 1] for o in outs], axis=0)
        t = jnp.concatenate(terms, axis=0)
        hi = t.astype(BF16)
        rest = t - hi.astype(F32)
        mid = rest.astype(BF16)
        low = (rest - mid.astype(F32)).astype(BF16)
        k_at = lax.broadcasted_iota(jnp.int32, (width, 128), 0)
        l_at = lax.broadcasted_iota(jnp.int32, (width, 128), 1)
        fold = jnp.where(k_at // part == l_at, 1.0, 0.0).astype(BF16)
        sums = sum(jnp.dot(p, fold, preferred_element_type=F32) for p in (hi, mid, low))
        lanes = sums[0:8]
        for s in range(1, capacity):
            lanes = lanes + pltpu.roll(sums[8 * s : 8 * s + 8], experts * s, 1)
        for i in range(PER):
            msg[4 * c + i] = lanes[2 * i : 2 * i + 1]
        weighted = (gate3 * hid).reshape(rows256, width).T.astype(BF16)
        step = 512
        for m in range(model // step):
            cols = pl.ds(m * step, step)
            piece = xall[c, :, :, cols].reshape(rows256, step)
            dwacc[:, cols] += jnp.dot(weighted, piece, preferred_element_type=F32)
        for i in range(PER):
            def put(i=i):
                pltpu.make_async_remote_copy(
                    src_ref=msg.at[4 * c + i], dst_ref=rbuf.at[4 * c + i],
                    send_sem=ms_sem.at[0], recv_sem=mr_sem.at[0],
                    device_id=(group_of(n, i), ep), device_id_type=MESH,
                ).start()
            if i == 0:
                pl.when(n > 0)(put)

                @pl.when(n == 0)
                def _():
                    rbuf[16] = msg[16]
            else:
                put()

    fetch(0)

    def step(n, carry):
        for back, stage in enumerate((stage1, stage2, stage3, stage4, stage5)):
            @pl.when((n >= back) & (n < CHUNKS + back))
            def _(back=back, stage=stage):
                stage(chunk_of(n - back)[0])

        @pl.when(n < CHUNKS - 1)
        def _():
            fetch(n + 1)

        @pl.when(n >= 5)
        def _():
            compute(n - 5)
        return carry

    lax.fori_loop(0, CHUNKS + 5, step, 0)
    dw_ref[...] = dwacc[...].astype(BF16)

    mine = xall[4, :, :, pl.ds(model, 128)].astype(F32).reshape(rows256, 128) > 0
    at_row = lax.broadcasted_iota(jnp.int32, (rows256, 128), 0)
    counts = []
    for r in range(2):
        before = mine & (at_row % 8 < 2) & (at_row < ep * 8 + r)
        counts.append(jnp.sum(jnp.where(before, 1.0, 0.0), axis=0, keepdims=True))

    most = rbuf.at[pl.ds(0, NZ - 1)]
    pltpu.make_async_copy(most, most, mr_sem.at[0]).wait()
    total = jnp.sum(rbuf[...], axis=0)
    s_at = lax.broadcasted_iota(jnp.int32, (8, 128), 0)
    l_at = lax.broadcasted_iota(jnp.int32, (8, 128), 1)
    spread = jnp.where(l_at // experts == s_at, total, 0.0)
    a_at = lax.broadcasted_iota(jnp.int32, (128, 128), 0)
    b_at = lax.broadcasted_iota(jnp.int32, (128, 128), 1)
    place = jnp.where(b_at == experts * ep + a_at % experts, 1.0, 0.0)
    fbuf[ep] = jnp.dot(spread, place, preferred_element_type=F32, precision=lax.Precision.HIGHEST)

    def tell(d, carry):
        pltpu.make_async_remote_copy(
            src_ref=fbuf.at[ep], dst_ref=fbuf.at[ep], send_sem=fs_sem.at[0], recv_sem=fr_sem.at[0],
            device_id=(z, (ep + d) % NE), device_id_type=MESH,
        ).start()
        return carry

    lax.fori_loop(1, NE, tell, 0)
    most = fbuf.at[pl.ds(0, NE - 1)]
    pltpu.make_async_copy(most, most, fr_sem.at[0]).wait()
    table = jnp.sum(fbuf[...], axis=0)
    vals = []
    for r in range(2):
        v = jnp.zeros((1, 128), F32)
        for s in range(capacity):
            v = jnp.where(counts[r] == float(s), table[s : s + 1], v)
        vals.append(v)
    val_ref[...] = jnp.concatenate(vals, axis=0)

    sent = zbuf.at[pl.ds(0, NZ - 1)]
    pltpu.make_async_copy(sent, sent, zs_sem.at[0]).wait()
    for c in range(CHUNKS):
        sent = xall.at[c, pl.ds(0, NE - 1)]
        pltpu.make_async_copy(sent, sent, s_sem.at[c]).wait()
    sent = msg.at[pl.ds(0, NZ - 1)]
    pltpu.make_async_copy(sent, sent, ms_sem.at[0]).wait()
    sent = fbuf.at[pl.ds(0, NE - 1)]
    pltpu.make_async_copy(sent, sent, fs_sem.at[0]).wait()


def per_device(out_grad, expert_ids, gate_values, hidden, w_down):
    groups, experts, capacity, part = hidden.shape
    model = out_grad.shape[1]
    width = experts * part
    named = expert_ids[:, :, None] == jnp.arange(128, dtype=jnp.int32)[None, None, :]
    gates = jnp.sum(jnp.where(named, gate_values[:, :, None], 0.0), axis=1)
    own = jnp.concatenate([out_grad, gates.astype(BF16)], axis=1)
    hid = jnp.transpose(hidden, (0, 2, 1, 3)).reshape(groups, capacity, width)
    vmem = pl.BlockSpec(memory_space=pltpu.VMEM)
    hid_grad, weight_grad, values = pl.pallas_call(
        kernel,
        out_shape=(
            jax.ShapeDtypeStruct((groups, capacity, width), F32),
            jax.ShapeDtypeStruct((width, model), BF16),
            jax.ShapeDtypeStruct((2, 128), F32),
        ),
        in_specs=[vmem] * 3,
        out_specs=(vmem,) * 3,
        scratch_shapes=[
            pltpu.VMEM((NZ, 2, LANES), BF16),
            pltpu.VMEM((CHUNKS, NE, 8, LANES), BF16),
            pltpu.VMEM((width, model), F32),
            pltpu.VMEM((NZ, 1, 128), F32),
            pltpu.VMEM((NZ, 1, 128), F32),
            pltpu.VMEM((NE, 8, 128), F32),
            pltpu.SemaphoreType.DMA((1,)),
            pltpu.SemaphoreType.DMA((NZ,)),
            pltpu.SemaphoreType.DMA((CHUNKS,)),
            pltpu.SemaphoreType.DMA((CHUNKS, 2, 16)),
            pltpu.SemaphoreType.DMA((CHUNKS,)),
            pltpu.SemaphoreType.DMA((1,)),
            pltpu.SemaphoreType.DMA((1,)),
            pltpu.SemaphoreType.DMA((1,)),
            pltpu.SemaphoreType.DMA((1,)),
        ],
        compiler_params=pltpu.CompilerParams(
            collective_id=0, has_side_effects=True, vmem_limit_bytes=56 * 1024 * 1024
        ),
    )(own, hid, w_down.reshape(width, model))
    hid_grad = hid_grad.astype(BF16).reshape(groups, capacity, experts, part)
    picked = jnp.where(named, values[:, None, :], 0.0)
    return (
        jnp.transpose(hid_grad, (0, 2, 1, 3)),
        weight_grad.reshape(experts, part, model),
        jnp.sum(picked, axis=2),
    )


def solution(mesh):
    placed = (
        P(("ctx", "ep"), None),
        P(("ctx", "ep"), None),
        P(("ctx", "ep"), None),
        P(None, "ep", None, "ctx"),
        P("ep", "ctx", None),
    )
    return jax.shard_map(
        per_device,
        mesh=mesh,
        in_specs=placed,
        out_specs=(P(None, "ep", None, "ctx"), P("ep", "ctx", None), P(("ctx", "ep"), None)),
        check_vma=False,
    )
```

```python
import jax
import jax.numpy as jnp
from jax import lax
from jax.experimental import pallas as pl
from jax.experimental.pallas import tpu as pltpu
from jax.sharding import PartitionSpec as P

MESH = pl.DeviceIdType.MESH
F32, BF16 = jnp.float32, jnp.bfloat16

NZ = 32
NE = 32
CHUNKS, PER = 8, 4
LANES = 3584 + 128
COLOURS = (
    ((0, 1920), (0, 1024), (1024, 896)),
    ((1920, 1792), (1920, 896), (2816, 896)),
)


ORDER = (4, 0, 5, 6, 2, 7, 3, 1)


def kernel(
    rows_hbm, ids_hbm, gates_hbm, hid_hbm, w_hbm,
    hg_ref, dw_ref, gg_ref,
    zbuf, xall, dwacc, msg, rbuf, fbuf,
    ids_ref, gates_ref, hid_ref, w_ref, pick_ref, earlier_ref,
    zs_sem, zr_sem, s_sem, r_sem, d_sem, ms_sem, mr_sem, fs_sem, fr_sem, io_sem,
):
    model = rows_hbm.shape[1]
    loads = [
        pltpu.make_async_copy(src, dst, io_sem.at[i])
        for i, (src, dst) in enumerate((
            (rows_hbm, zbuf.at[16, :, pl.ds(0, model)]), (ids_hbm, ids_ref), (gates_hbm, gates_ref),
            (hid_hbm, hid_ref), (w_hbm, w_ref),
        ))
    ]
    for load in loads:
        load.start()
    z, ep = lax.axis_index("ctx"), lax.axis_index("ep")
    core, px, py = ep % 2, ep // 8, (ep // 2) % 4
    experts, capacity = 4, hid_ref.shape[1]
    width = w_ref.shape[0]
    part = width // experts

    def along_z(d):
        return ((z + d + NZ) % NZ, ep)

    def chip(x, y):
        return ((x + 4) % 4 * 4 + (y + 4) % 4) * 2 + core

    def at(colour, dp, dq):
        return chip(px + dq, py + dp) if colour == 0 else chip(px + dp, py + dq)

    partner = (z, ep + 1 - 2 * core)

    barrier = pltpu.get_barrier_semaphore()
    near = [along_z(d) for d in (1, 2, 3, 4, -1, -2, -3, -4)]
    near += [(z, at(0, 1, 0)), (z, at(0, -1, 0)), (z, at(0, 0, 1)), (z, at(0, 0, -1)), partner]
    for peer in near:
        pl.semaphore_signal(barrier, inc=1, device_id=peer, device_id_type=MESH)
    for load in loads[:3]:
        load.wait()
    ids = ids_ref[...]
    e_lane = lax.broadcasted_iota(jnp.int32, (2, 128), 1)
    spread = jnp.zeros((2, 128), F32)
    for k in range(ids.shape[1]):
        spread = jnp.where(e_lane == ids[:, k : k + 1], gates_ref[:, k : k + 1], spread)
    zbuf[16, :, pl.ds(model, 128)] = spread.astype(BF16)

    pl.semaphore_wait(barrier, len(near))

    def z_send(src, slot, d):
        pltpu.make_async_remote_copy(
            src_ref=src, dst_ref=zbuf.at[slot], send_sem=zs_sem.at[0], recv_sem=zr_sem.at[slot],
            device_id=along_z(d), device_id_type=MESH,
        ).start()

    own = zbuf.at[16]
    for j in (4, 3, 2, 1):
        z_send(own, j - 1, j)
        z_send(own, 16 + j, -j)
    dwacc[...] = jnp.zeros_like(dwacc)
    rows256 = NE * 2 * PER
    e_at = lax.broadcasted_iota(jnp.int32, (128, width), 0)
    f_at = lax.broadcasted_iota(jnp.int32, (128, width), 1)
    pick_ref[...] = jnp.where(e_at == experts * ep + f_at // part, 1.0, 0.0).astype(BF16)
    r_at = lax.broadcasted_iota(jnp.int32, (rows256, rows256), 0)
    c_at = lax.broadcasted_iota(jnp.int32, (rows256, rows256), 1)
    earlier = ((r_at % 8) // 2 == (c_at % 8) // 2) & (c_at < r_at)
    earlier_ref[...] = jnp.where(earlier, 1.0, 0.0).astype(BF16)

    def z_wait(slot):
        pltpu.make_async_copy(own, zbuf.at[slot], zr_sem.at[slot]).wait()

    def chunk_of(n):
        c = 0
        for i, one in enumerate(ORDER):
            c = c + jnp.where(n == i, one, 0)
        return c

    def group_of(c, i):
        up, w = c // 4, c % 4
        return (z + 2 * NZ + up * (4 * w + i) - (1 - up) * (4 * w + i + 1)) % NZ

    def forward(w):
        low, high = 4 * w + 3, 20 + 4 * w
        z_wait(low)
        z_wait(high)
        for j in (4, 3, 2, 1):
            z_send(zbuf.at[low], low + j, j)
            if high + j < 32:
                z_send(zbuf.at[high], high + j, -j)

    def fetch(n):
        c = ORDER[n]
        if c < 4:
            slots = [4 * c + i for i in range(4 if c == 3 else 3)]
        else:
            slots = [4 * c + i for i in (1, 2, 3)]
        for slot in slots:
            z_wait(slot)
        rows = [zbuf[4 * c + i].astype(F32) for i in range(PER)]
        xall[c, ep] = jnp.concatenate(rows, axis=0).astype(BF16)

    def block(c, e, lanes):
        return xall.at[c, e, :, pl.ds(*lanes)]

    def send(c, e, lanes, to, sem):
        pltpu.make_async_remote_copy(
            src_ref=block(c, e, lanes), dst_ref=block(c, e, lanes), send_sem=s_sem.at[c], recv_sem=sem,
            device_id=to, device_id_type=MESH,
        ).start()

    def share(c, colour, dp, dq):
        send(c, at(colour, dp, dq), COLOURS[colour][0], partner, d_sem.at[c])

    def send_p(c, colour, dp, dq, step, piece):
        send(c, at(colour, dp, dq), COLOURS[colour][piece], (z, at(colour, step, 0)),
             r_sem.at[c, colour, (dp - step) % 4 * 4 + dq % 4])

    def send_q(c, colour, dp, dq, step, piece):
        send(c, at(colour, dp, dq), COLOURS[colour][piece], (z, at(colour, 0, step)),
             r_sem.at[c, colour, dp % 4 * 4 + (dq - step) % 4])

    def wait(c, colour, dp, dq):
        ref = block(c, at(colour, dp, dq), COLOURS[colour][0])
        pltpu.make_async_copy(ref, ref, r_sem.at[c, colour, dp % 4 * 4 + dq % 4]).wait()

    def stage1(c):
        for colour in (0, 1):
            send_p(c, colour, 0, 0, 1, 0)
            send_p(c, colour, 0, 0, -1, 0)
        for colour in (0, 1):
            share(c, colour, 0, 0)

    def stage2(c):
        for colour in (0, 1):
            for dp in (-1, 1):
                wait(c, colour, dp, 0)
                send_p(c, colour, dp, 0, -dp, 1 if dp < 0 else 2)
        for colour in (0, 1):
            for dp in (0, -1, 1):
                send_q(c, colour, dp, 0, 1, 0)
                send_q(c, colour, dp, 0, -1, 0)
        for colour in (0, 1):
            for dp in (-1, 1):
                share(c, colour, dp, 0)

    def stage3(c):
        for colour in (0, 1):
            wait(c, colour, 2, 0)
            send_q(c, colour, 2, 0, 1, 0)
            send_q(c, colour, 2, 0, -1, 0)
        for dp in (0, -1, 1):
            for colour in (0, 1):
                for dq in (-1, 1):
                    wait(c, colour, dp, dq)
                    send_q(c, colour, dp, dq, -dq, 1 if dq < 0 else 2)
        for colour in (0, 1):
            share(c, colour, 2, 0)
            for dp in (0, -1, 1):
                for dq in (-1, 1):
                    share(c, colour, dp, dq)

    def stage4(c):
        for colour in (0, 1):
            for dq in (-1, 1):
                wait(c, colour, 2, dq)
                send_q(c, colour, 2, dq, -dq, 1 if dq < 0 else 2)
        for colour in (0, 1):
            for dp in (0, -1, 1):
                wait(c, colour, dp, 2)
                share(c, colour, dp, 2)
            for dq in (-1, 1):
                share(c, colour, 2, dq)

    def stage5(c):
        for colour in (0, 1):
            wait(c, colour, 2, 2)
            share(c, colour, 2, 2)

    def compute(n):
        c = chunk_of(n)

        @pl.when(n == 0)
        def _():
            loads[3].wait()
            loads[4].wait()

        half = xall.at[c, pl.ds(0, NE // 2)]
        pltpu.make_async_copy(half, half, d_sem.at[c]).wait()
        gates = xall[c, :, :, pl.ds(model, 128)].reshape(rows256, 128)
        gate = jnp.dot(gates, pick_ref[...], preferred_element_type=F32)
        live = gate > 0
        slot = jnp.dot(earlier_ref[...], jnp.where(live, 1.0, 0.0).astype(BF16), preferred_element_type=F32)
        slot = jnp.where(live, slot, -1.0).reshape(NE, 8, width)
        rows = xall[c, :, :, pl.ds(0, model)].reshape(rows256, model)
        grad_in = lax.dot_general(rows, w_ref[...], (((1,), (1,)), ((), ())), preferred_element_type=F32)
        own_group = []
        for i in range(PER):
            h = hid_ref[group_of(c, i)].astype(F32)
            own_group.append(jnp.concatenate([h[:, j, :] for j in range(experts)], axis=1))
        row8 = lax.broadcasted_iota(jnp.int32, (8, width), 0) // 2
        hid = jnp.zeros((NE, 8, width), F32)
        for s in range(capacity):
            wide = jnp.zeros((8, width), F32)
            for i in range(PER):
                wide = jnp.where(row8 == i, own_group[i][s : s + 1, :], wide)
            hid = jnp.where(slot == float(s), wide[None], hid)
        grad3 = grad_in.reshape(NE, 8, width)
        gate3 = gate.reshape(NE, 8, width)
        term = hid * grad3
        terms = []
        for s in range(capacity):
            t = jnp.sum(jnp.where(slot == float(s), term, 0.0), axis=0)
            terms.append(t + pltpu.roll(t, 7, 0))
        t = jnp.concatenate(terms, axis=0)
        hi = t.astype(BF16)
        rest = t - hi.astype(F32)
        mid = rest.astype(BF16)
        low = (rest - mid.astype(F32)).astype(BF16)
        k_at = lax.broadcasted_iota(jnp.int32, (width, 128), 0)
        l_at = lax.broadcasted_iota(jnp.int32, (width, 128), 1)
        fold = jnp.where(k_at // part == l_at, 1.0, 0.0).astype(BF16)
        sums = sum(jnp.dot(p, fold, preferred_element_type=F32) for p in (hi, mid, low))
        lanes = sums[0:8]
        for s in range(1, capacity):
            lanes = lanes + pltpu.roll(sums[8 * s : 8 * s + 8], experts * s, 1)
        for i in range(PER):
            msg[4 * c + i] = lanes[2 * i : 2 * i + 1]
        out = (gate3 * grad3).astype(BF16).astype(F32)
        outs = []
        for s in range(capacity):
            o = jnp.sum(jnp.where(slot == float(s), out, 0.0), axis=0)
            outs.append(o + pltpu.roll(o, 7, 0))
        for i in range(PER):
            o = jnp.concatenate([o[2 * i : 2 * i + 1] for o in outs], axis=0)
            o = jnp.stack([o[:, j * part : (j + 1) * part] for j in range(experts)], axis=1)
            hg_ref[group_of(c, i)] = o.astype(BF16)
        weighted = (gate3 * hid).reshape(rows256, width).T.astype(BF16)
        for i in range(PER):
            def put(i=i):
                pltpu.make_async_remote_copy(
                    src_ref=msg.at[4 * c + i], dst_ref=rbuf.at[4 * c + i],
                    send_sem=ms_sem.at[0], recv_sem=mr_sem.at[0],
                    device_id=(group_of(c, i), ep), device_id_type=MESH,
                ).start()
            if i == 0:
                pl.when(n > 0)(put)

                @pl.when(n == 0)
                def _():
                    rbuf[16] = msg[16]
            else:
                put()
        step = 512
        for m in range(model // step):
            cols = pl.ds(m * step, step)
            piece = xall[c, :, :, cols].reshape(rows256, step)
            dwacc[:, cols] += jnp.dot(weighted, piece, preferred_element_type=F32)

    fetch(0)
    forward(0)

    def step(n, carry):
        def run(back, stage):
            @pl.when((n >= back) & (n < CHUNKS + back))
            def _():
                stage(chunk_of(n - back))

        run(0, stage1)
        run(1, stage2)
        run(4, stage5)
        run(2, stage3)
        run(3, stage4)

        for i in range(CHUNKS - 1):
            @pl.when(n == i)
            def _(i=i):
                fetch(i + 1)
                if i in (1, 2):
                    forward(i)

        @pl.when(n >= 4)
        def _():
            compute(n - 4)

        return carry

    lax.fori_loop(0, CHUNKS + 4, step, 0)
    dw_ref[...] = dwacc[...].astype(BF16)

    mine = xall[4, :, :, pl.ds(model, 128)].astype(F32).reshape(rows256, 128) > 0
    at_row = lax.broadcasted_iota(jnp.int32, (rows256, 128), 0)
    counts = []
    for r in range(2):
        before = mine & (at_row % 8 < 2) & (at_row < ep * 8 + r)
        counts.append(jnp.sum(jnp.where(before, 1.0, 0.0), axis=0, keepdims=True))

    most = rbuf.at[pl.ds(0, NZ - 1)]
    pltpu.make_async_copy(most, most, mr_sem.at[0]).wait()
    total = jnp.sum(rbuf[...], axis=0)
    s_at = lax.broadcasted_iota(jnp.int32, (8, 128), 0)
    l_at = lax.broadcasted_iota(jnp.int32, (8, 128), 1)
    spread = jnp.where(l_at // experts == s_at, total, 0.0)
    a_at = lax.broadcasted_iota(jnp.int32, (128, 128), 0)
    b_at = lax.broadcasted_iota(jnp.int32, (128, 128), 1)
    place = jnp.where(b_at == experts * ep + a_at % experts, 1.0, 0.0)
    fbuf[ep] = jnp.dot(spread, place, preferred_element_type=F32, precision=lax.Precision.HIGHEST)

    def tell(d, carry):
        pltpu.make_async_remote_copy(
            src_ref=fbuf.at[ep], dst_ref=fbuf.at[ep], send_sem=fs_sem.at[0], recv_sem=fr_sem.at[0],
            device_id=(z, (ep + d) % NE), device_id_type=MESH,
        ).start()
        return carry

    lax.fori_loop(1, NE, tell, 0)
    most = fbuf.at[pl.ds(0, NE - 1)]
    pltpu.make_async_copy(most, most, fr_sem.at[0]).wait()
    table = jnp.sum(fbuf[...], axis=0)
    vals = []
    for r in range(2):
        v = jnp.zeros((1, 128), F32)
        for s in range(capacity):
            v = jnp.where(counts[r] == float(s), table[s : s + 1], v)
        vals.append(v)
    val = jnp.concatenate(vals, axis=0)
    k_lane = lax.broadcasted_iota(jnp.int32, (2, 8), 1)
    gg = jnp.zeros((2, 8), F32)
    for k in range(ids.shape[1]):
        one = jnp.sum(jnp.where(e_lane == ids[:, k : k + 1], val, 0.0), axis=1, keepdims=True)
        gg = jnp.where(k_lane == k, one, gg)
    gg_ref[...] = gg

    sent = zbuf.at[pl.ds(0, NZ - 1)]
    pltpu.make_async_copy(sent, sent, zs_sem.at[0]).wait()
    for c in range(CHUNKS):
        sent = xall.at[c, pl.ds(0, NE - 1)]
        pltpu.make_async_copy(sent, sent, s_sem.at[c]).wait()
    sent = msg.at[pl.ds(0, NZ - 1)]
    pltpu.make_async_copy(sent, sent, ms_sem.at[0]).wait()
    sent = fbuf.at[pl.ds(0, NE - 1)]
    pltpu.make_async_copy(sent, sent, fs_sem.at[0]).wait()


def per_device(out_grad, expert_ids, gate_values, hidden, w_down):
    groups, experts, capacity, part = hidden.shape
    model = out_grad.shape[1]
    width = experts * part
    width = experts * part
    vmem = pl.BlockSpec(memory_space=pltpu.VMEM)
    hbm = pl.BlockSpec(memory_space=pltpu.HBM)
    hid_grad, weight_grad, gate_grad = pl.pallas_call(
        kernel,
        out_shape=(
            jax.ShapeDtypeStruct((groups, capacity, experts, part), BF16),
            jax.ShapeDtypeStruct((width, model), BF16),
            jax.ShapeDtypeStruct((2, 8), F32),
        ),
        in_specs=[hbm] * 5,
        out_specs=(vmem,) * 3,
        scratch_shapes=[
            pltpu.VMEM((NZ, 2, LANES), BF16),
            pltpu.VMEM((CHUNKS, NE, 8, LANES), BF16),
            pltpu.VMEM((width, model), F32),
            pltpu.VMEM((NZ, 1, 128), F32),
            pltpu.VMEM((NZ, 1, 128), F32),
            pltpu.VMEM((NE, 8, 128), F32),
            pltpu.VMEM(expert_ids.shape, jnp.int32),
            pltpu.VMEM(gate_values.shape, F32),
            pltpu.VMEM((groups, capacity, experts, part), BF16),
            pltpu.VMEM((width, model), BF16),
            pltpu.VMEM((128, width), BF16),
            pltpu.VMEM((NE * 2 * PER, NE * 2 * PER), BF16),
            pltpu.SemaphoreType.DMA((1,)),
            pltpu.SemaphoreType.DMA((NZ,)),
            pltpu.SemaphoreType.DMA((CHUNKS,)),
            pltpu.SemaphoreType.DMA((CHUNKS, 2, 16)),
            pltpu.SemaphoreType.DMA((CHUNKS,)),
            pltpu.SemaphoreType.DMA((1,)),
            pltpu.SemaphoreType.DMA((1,)),
            pltpu.SemaphoreType.DMA((1,)),
            pltpu.SemaphoreType.DMA((1,)),
            pltpu.SemaphoreType.DMA((5,)),
        ],
        compiler_params=pltpu.CompilerParams(
            collective_id=0, has_side_effects=True, vmem_limit_bytes=40 * 1024 * 1024
        ),
    )(*(
        pltpu.with_memory_space_constraint(one, pltpu.HBM)
        for one in (
            out_grad, expert_ids, gate_values,
            jnp.transpose(hidden, (0, 2, 1, 3)), w_down.reshape(width, model),
        )
    ))
    return (
        jnp.transpose(hid_grad, (0, 2, 1, 3)),
        weight_grad.reshape(experts, part, model),
        gate_grad,
    )


def solution(mesh):
    placed = (
        P(("ctx", "ep"), None),
        P(("ctx", "ep"), None),
        P(("ctx", "ep"), None),
        P(None, "ep", None, "ctx"),
        P("ep", "ctx", None),
    )
    return jax.shard_map(
        per_device,
        mesh=mesh,
        in_specs=placed,
        out_specs=(P(None, "ep", None, "ctx"), P("ep", "ctx", None), P(("ctx", "ep"), None)),
        check_vma=False,
    )
```
